16 devices in a mesh: dp: 2 (over y, z), tp: 8 (over x, core).
Axes of the slice: x: 4, y: 2, z: 1, core: 2. Of those that a mesh axis runs over, the one named last changes fastest.
The devices are a block of a 4x4x8 slice.
Arguments:
- x_steps: bfloat16 [16, 128, 4096], P(None, 'dp'), parts along dimension 1
- cur_len: int32 [128], P('dp'), parts along dimension 0
- k_cache: bfloat16 [2, 128, 64, 16, 256], P(None, 'dp', None, 'tp'), parts along dimension 1
- v_cache: bfloat16 [2, 128, 64, 16, 256], P(None, 'dp', None, 'tp'), parts along dimension 1
- ln_gain: bfloat16 [2, 4096], replicated
- ln_bias: bfloat16 [2, 4096], replicated
- w_q: bfloat16 [2, 4096, 4096], P(None, None, 'tp')
- w_k: bfloat16 [2, 4096, 4096], P(None, None, 'tp')
- w_v: bfloat16 [2, 4096, 4096], P(None, None, 'tp')
- w_o: bfloat16 [2, 4096, 4096], P(None, 'tp')
- w_in: bfloat16 [2, 4096, 16384], P(None, None, 'tp')
- b_in: bfloat16 [2, 16384], P(None, 'tp')
- w_out: bfloat16 [2, 16384, 4096], P(None, 'tp')
- b_out: bfloat16 [2, 4096], replicated
Outputs:
- output 1: bfloat16 [16, 128, 4096], P(None, 'dp'), parts along dimension 1
- output 2: bfloat16 [2, 128, 64, 16, 256], P(None, 'dp', None, 'tp'), parts along dimension 1
- output 3: bfloat16 [2, 128, 64, 16, 256], P(None, 'dp', None, 'tp'), parts along dimension 1
There are 2 independent parts. The reference program is written for one: setup_inputs(seed, part) draws one part's arguments, and reference() takes and returns one part's arrays. A program takes and returns all parts, laid end to end along the dimension named above; an argument that names none is the same for every part.
All inputs are finite; a program needn't handle non-finite values.
Results may differ from the reference program's by a relative error of at most 0.0170477.
Values are sent between devices in bfloat16 or wider.
A program may use at most 768 MiB of HBM per device.

```python
import jax
import jax.numpy as jnp
from jax import lax

D_MODEL = 4096
N_HEADS = 16
HEAD_DIM = 256
ROT_DIM = 64
FF_DIM = 16384
BATCH_PART = 64
CACHE_LEN = 64
N_STEPS = 16
N_LAYERS = 2
LN_EPS = 1e-5
QUERY_GAIN = 2.5


def setup_inputs(seed: int = 0, part: int = 0) -> dict:
    base_key = jax.random.key(seed)
    shared_keys = jax.random.split(base_key, 10)
    part_keys = jax.random.split(jax.random.fold_in(base_key, part), 6)
    scale_model = D_MODEL ** -0.5
    scale_ff = FF_DIM ** -0.5
    cache_shape = (N_LAYERS, BATCH_PART, CACHE_LEN, N_HEADS, HEAD_DIM)

    def gaussian(key, shape, scale):
        return jax.random.normal(key, shape, jnp.float32) * scale

    top_len = CACHE_LEN - N_STEPS
    raw_span = jax.random.randint(part_keys[1], (BATCH_PART,), 0, top_len)
    shift_bits = jax.random.randint(part_keys[2], (BATCH_PART,), 0, 8)
    full_row = jax.random.randint(part_keys[3], (), 0, BATCH_PART)
    cur_len = 1 + jnp.right_shift(raw_span, shift_bits)
    cur_len = jnp.where(jnp.arange(BATCH_PART) == full_row, top_len, cur_len).astype(jnp.int32)
    return {
        "x_steps": gaussian(part_keys[0], (N_STEPS, BATCH_PART, D_MODEL), 1.0).astype(jnp.bfloat16),
        "cur_len": cur_len,
        "k_cache": gaussian(part_keys[4], cache_shape, 1.0).astype(jnp.bfloat16),
        "v_cache": gaussian(part_keys[5], cache_shape, 1.0).astype(jnp.bfloat16),
        "ln_gain": (1.0 + gaussian(shared_keys[0], (N_LAYERS, D_MODEL), 0.2)).astype(jnp.bfloat16),
        "ln_bias": gaussian(shared_keys[1], (N_LAYERS, D_MODEL), 0.2).astype(jnp.bfloat16),
        "w_q": gaussian(shared_keys[2], (N_LAYERS, D_MODEL, D_MODEL), QUERY_GAIN * scale_model).astype(jnp.bfloat16),
        "w_k": gaussian(shared_keys[3], (N_LAYERS, D_MODEL, D_MODEL), scale_model).astype(jnp.bfloat16),
        "w_v": gaussian(shared_keys[4], (N_LAYERS, D_MODEL, D_MODEL), scale_model).astype(jnp.bfloat16),
        "w_o": gaussian(shared_keys[5], (N_LAYERS, D_MODEL, D_MODEL), scale_model).astype(jnp.bfloat16),
        "w_in": gaussian(shared_keys[6], (N_LAYERS, D_MODEL, FF_DIM), scale_model).astype(jnp.bfloat16),
        "b_in": gaussian(shared_keys[7], (N_LAYERS, FF_DIM), 0.5).astype(jnp.bfloat16),
        "w_out": gaussian(shared_keys[8], (N_LAYERS, FF_DIM, D_MODEL), scale_ff).astype(jnp.bfloat16),
        "b_out": gaussian(shared_keys[9], (N_LAYERS, D_MODEL), 0.3).astype(jnp.bfloat16),
    }


def layer_norm(hidden, gain, bias):
    hid_f32 = hidden.astype(jnp.float32)
    row_mean = jnp.mean(hid_f32, axis=-1, keepdims=True)
    centered = hid_f32 - row_mean
    row_var = jnp.mean(centered * centered, axis=-1, keepdims=True)
    normed = centered / jnp.sqrt(row_var + LN_EPS)
    return (normed * gain.astype(jnp.float32) + bias.astype(jnp.float32)).astype(jnp.bfloat16)


def rotary_tables(positions):
    inv_freq = 1.0 / (10000.0 ** (jnp.arange(0, ROT_DIM, 2).astype(jnp.float32) / ROT_DIM))
    angles = positions.astype(jnp.float32)[:, None] * inv_freq[None, :]
    return jnp.cos(angles)[:, None, :], jnp.sin(angles)[:, None, :]


def apply_rotary(vectors, cos_tab, sin_tab):
    lead_shape = vectors.shape[:-1]
    pairs = vectors[..., :ROT_DIM].reshape(lead_shape + (ROT_DIM // 2, 2))
    even_part = pairs[..., 0]
    odd_part = pairs[..., 1]
    rotated = jnp.stack([even_part * cos_tab - odd_part * sin_tab, odd_part * cos_tab + even_part * sin_tab], axis=-1)
    return jnp.concatenate([rotated.reshape(lead_shape + (ROT_DIM,)), vectors[..., ROT_DIM:]], axis=-1)


def decoder_layer(hidden, new_pos, layer):
    (k_layer, v_layer, gain, bias, q_weight, k_weight, v_weight, o_weight,
     in_weight, in_bias, out_weight, out_bias) = layer
    batch = hidden.shape[0]
    head_shape = (batch, N_HEADS, HEAD_DIM)
    normed = layer_norm(hidden, gain, bias)
    query = jnp.dot(normed, q_weight, preferred_element_type=jnp.float32).reshape(head_shape)
    key_new = jnp.dot(normed, k_weight, preferred_element_type=jnp.float32).reshape(head_shape)
    value_new = jnp.dot(normed, v_weight, preferred_element_type=jnp.float32).reshape(head_shape).astype(jnp.bfloat16)
    cos_tab, sin_tab = rotary_tables(new_pos)
    query = apply_rotary(query, cos_tab, sin_tab).astype(jnp.bfloat16)
    key_new = apply_rotary(key_new, cos_tab, sin_tab).astype(jnp.bfloat16)
    slot_ids = jnp.arange(CACHE_LEN)
    written = (slot_ids[None, :] == new_pos[:, None])[:, :, None, None]
    k_layer = jnp.where(written, key_new[:, None], k_layer)
    v_layer = jnp.where(written, value_new[:, None], v_layer)
    scores = jnp.einsum("bhe,bshe->bhs", query.astype(jnp.float32), k_layer.astype(jnp.float32)) * (HEAD_DIM ** -0.5)
    visible = (slot_ids[None, :] <= new_pos[:, None])[:, None, :]
    scores = jnp.where(visible, scores, -jnp.inf)
    exp_scores = jnp.exp(scores - jnp.max(scores, axis=-1, keepdims=True))
    attn_probs = (exp_scores / jnp.sum(exp_scores, axis=-1, keepdims=True)).astype(jnp.bfloat16)
    context = jnp.einsum("bhs,bshe->bhe", attn_probs.astype(jnp.float32), v_layer.astype(jnp.float32))
    context = context.astype(jnp.bfloat16).reshape(batch, N_HEADS * HEAD_DIM)
    attn_out = jnp.dot(context, o_weight, preferred_element_type=jnp.float32)
    pre_act = jnp.dot(normed, in_weight, preferred_element_type=jnp.float32) + in_bias.astype(jnp.float32)
    gelu_act = jax.nn.gelu(pre_act, approximate=True).astype(jnp.bfloat16)
    mlp_out = jnp.dot(gelu_act, out_weight, preferred_element_type=jnp.float32)
    new_hidden = (hidden.astype(jnp.float32) + attn_out + mlp_out + out_bias.astype(jnp.float32)).astype(jnp.bfloat16)
    return new_hidden, (k_layer, v_layer)


def reference(x_steps, cur_len, k_cache, v_cache, ln_gain, ln_bias, w_q, w_k, w_v, w_o, w_in, b_in, w_out, b_out):
    def one_step(caches, step_in):
        x_now, step_idx = step_in
        new_pos = cur_len + step_idx

        def layer_step(hidden, layer):
            return decoder_layer(hidden, new_pos, layer)

        layers = (caches[0], caches[1], ln_gain, ln_bias, w_q, w_k, w_v, w_o, w_in, b_in, w_out, b_out)
        last_hidden, new_caches = lax.scan(layer_step, x_now, layers)
        return new_caches, last_hidden

    final_caches, hidden_out = lax.scan(one_step, (k_cache, v_cache), (x_steps, jnp.arange(N_STEPS, dtype=jnp.int32)))
    return hidden_out, final_caches[0], final_caches[1]
```

```python
import jax
import jax.numpy as jnp
from jax import lax
from jax.sharding import PartitionSpec as P

ROT_DIM = 64
LN_EPS = 1e-5


def layer_norm(hidden, gain, bias):
    hid_f32 = hidden.astype(jnp.float32)
    row_mean = jnp.mean(hid_f32, axis=-1, keepdims=True)
    centered = hid_f32 - row_mean
    row_var = jnp.mean(centered * centered, axis=-1, keepdims=True)
    normed = centered * lax.rsqrt(row_var + LN_EPS)
    return (normed * gain.astype(jnp.float32) + bias.astype(jnp.float32)).astype(jnp.bfloat16)


def rotary_rows(positions, head_dim, n_heads):
    inv_freq = 1.0 / (10000.0 ** (jnp.arange(0, ROT_DIM, 2).astype(jnp.float32) / ROT_DIM))
    angles = positions.astype(jnp.float32)[:, None] * inv_freq[None, :]
    rows = positions.shape[0]
    cos_pair = jnp.repeat(jnp.cos(angles), 2, axis=1)
    sin_pair = jnp.repeat(jnp.sin(angles), 2, axis=1) * jnp.where(jnp.arange(ROT_DIM) % 2 == 0, -1.0, 1.0)[None, :]
    cos_head = jnp.concatenate([cos_pair, jnp.ones((rows, head_dim - ROT_DIM), jnp.float32)], axis=1)
    sin_head = jnp.concatenate([sin_pair, jnp.zeros((rows, head_dim - ROT_DIM), jnp.float32)], axis=1)
    return jnp.tile(cos_head, (1, n_heads)), jnp.tile(sin_head, (1, n_heads))


def apply_rotary(vectors, cos_tab, sin_tab):
    even = (jnp.arange(vectors.shape[-1]) % 2 == 0)[None, :]
    partner = jnp.where(even, jnp.roll(vectors, -1, axis=-1), jnp.roll(vectors, 1, axis=-1))
    return (vectors * cos_tab + partner * sin_tab).astype(jnp.bfloat16)


def decode_shard(x_steps, cur_len, k_cache, v_cache, ln_gain, ln_bias, w_q, w_k, w_v, w_o, w_in, b_in, w_out, b_out):
    n_steps, batch, d_model = x_steps.shape
    n_layers, _, cache_len, n_heads, head_dim = k_cache.shape
    rows = n_steps * batch
    steps = jnp.arange(n_steps)
    positions = cur_len[None, :] + steps[:, None]
    cos_tab, sin_tab = rotary_rows(positions.reshape(rows), head_dim, n_heads)
    slots = jnp.arange(cache_len)
    visible = slots[None, None, None, :] <= positions[:, :, None, None]
    place = slots[None, :, None] == positions.T[:, None, :]
    written = jnp.any(place, axis=2)[:, :, None, None]
    place = place.astype(jnp.bfloat16)

    def put(old, new):
        spread = jnp.einsum("bst,tbn->bsn", place, new.reshape(n_steps, batch, n_heads * head_dim),
                            preferred_element_type=jnp.float32).astype(jnp.bfloat16)
        return jnp.where(written, spread.reshape(old.shape), old)

    hidden = x_steps.reshape(rows, d_model)
    k_out, v_out = [], []
    for layer in range(n_layers):
        normed = layer_norm(hidden, ln_gain[layer], ln_bias[layer])
        query = jnp.dot(normed, w_q[layer], preferred_element_type=jnp.float32)
        key_new = jnp.dot(normed, w_k[layer], preferred_element_type=jnp.float32)
        value_new = jnp.dot(normed, w_v[layer], preferred_element_type=jnp.float32).astype(jnp.bfloat16)
        query = apply_rotary(query, cos_tab, sin_tab).reshape(n_steps, batch, n_heads, head_dim)
        key_new = apply_rotary(key_new, cos_tab, sin_tab)
        keys = put(k_cache[layer], key_new)
        values = put(v_cache[layer], value_new)
        k_out.append(keys)
        v_out.append(values)
        scores = jnp.einsum("tbhe,bshe->tbhs", query, keys, preferred_element_type=jnp.float32) * (head_dim ** -0.5)
        scores = jnp.where(visible, scores, -jnp.inf)
        exp_scores = jnp.exp(scores - jnp.max(scores, axis=-1, keepdims=True))
        probs = (exp_scores / jnp.sum(exp_scores, axis=-1, keepdims=True)).astype(jnp.bfloat16)
        context = jnp.einsum("tbhs,bshe->tbhe", probs, values, preferred_element_type=jnp.float32)
        context = context.astype(jnp.bfloat16).reshape(rows, n_heads * head_dim)
        pre_act = jnp.dot(normed, w_in[layer], preferred_element_type=jnp.float32) + b_in[layer].astype(jnp.float32)
        gelu_act = jax.nn.gelu(pre_act, approximate=True).astype(jnp.bfloat16)
        part = jnp.dot(context, w_o[layer], preferred_element_type=jnp.float32) + jnp.dot(
            gelu_act, w_out[layer], preferred_element_type=jnp.float32)
        total = lax.psum(part.astype(jnp.bfloat16), "tp")
        hidden = (hidden.astype(jnp.float32) + total.astype(jnp.float32) + b_out[layer].astype(jnp.float32)).astype(jnp.bfloat16)
    return hidden.reshape(n_steps, batch, d_model), jnp.stack(k_out), jnp.stack(v_out)


def solution(mesh):
    cache_spec = P(None, "dp", None, "tp", None)
    in_specs = (P(None, "dp", None), P("dp"), cache_spec, cache_spec, P(None, None), P(None, None),
                P(None, None, "tp"), P(None, None, "tp"), P(None, None, "tp"), P(None, "tp", None),
                P(None, None, "tp"), P(None, "tp"), P(None, "tp", None), P(None, None))
    out_specs = (P(None, "dp", None), cache_spec, cache_spec)
    return jax.shard_map(decode_shard, mesh=mesh, in_specs=in_specs, out_specs=out_specs, check_vma=False)
```
